16 devices in a mesh: dp: 4 (over y, z, core), tp: 4 (over x).
Axes of the slice: x: 4, y: 2, z: 1, core: 2. Of those that a mesh axis runs over, the one named last changes fastest.
The devices are a block of a 4x4x8 slice.
Arguments:
- x: bfloat16 [2560, 7168], P(('dp', 'tp')), parts along dimension 0
- w_gate: bfloat16 [7168, 20480], P(None, 'tp')
- w_up: bfloat16 [7168, 20480], P(None, 'tp')
- w_down: bfloat16 [20480, 7168], P('tp')
Outputs:
- output: bfloat16 [2560, 7168], P(('dp', 'tp')), parts along dimension 0
There are 4 independent parts. The reference program is written for one: setup_inputs(seed, part) draws one part's arguments, and reference() takes and returns one part's arrays. A program takes and returns all parts, laid end to end along the dimension named above; an argument that names none is the same for every part.
All inputs are finite; a program needn't handle non-finite values.
Results may differ from the reference program's by a relative error of at most 0.016.
Values are sent between devices in bfloat16 or wider.
A program may use at most 768 MiB of HBM per device.

```python
import jax
import jax.numpy as jnp

ROWS = 640
D = 7168
FF = 20480


def setup_inputs(seed: int = 0, part: int = 0) -> dict:
    kx, kg, ku, kd = jax.random.split(jax.random.key(seed), 4)
    drawn = {
        "x": jax.random.normal(jax.random.fold_in(kx, part), (ROWS, D), jnp.float32),
        "w_gate": jax.random.normal(kg, (D, FF), jnp.float32) * D**-0.5,
        "w_up": jax.random.normal(ku, (D, FF), jnp.float32) * D**-0.5,
        "w_down": jax.random.normal(kd, (FF, D), jnp.float32) * FF**-0.5,
    }
    return {k: v.astype(jnp.bfloat16) for k, v in drawn.items()}


def reference(x, w_gate, w_up, w_down):
    gate = jnp.dot(x, w_gate, preferred_element_type=jnp.float32)
    up = jnp.dot(x, w_up, preferred_element_type=jnp.float32)
    hidden = (jax.nn.silu(gate) * up).astype(jnp.bfloat16)
    return jnp.dot(hidden, w_down, preferred_element_type=jnp.float32).astype(jnp.bfloat16)
```

```python
import functools

import jax
import jax.numpy as jnp
from jax import lax
from jax.experimental import pallas as pl
from jax.experimental.pallas import tpu as pltpu
from jax.sharding import PartitionSpec as P

F32 = jnp.float32
BF16 = jnp.bfloat16
KC = 1024
NU = 512
RING = 20
COMM = True


def _kernel(
    x_ref, wg_ref, wu_ref, wd_ref, out_ref,
    xbuf, acc_g, acc_u, hid, wbuf, thru, own, obuf, rfar, rsum, rdir, sfar, ssum, sdir,
    wsem, xsem, osem, ag_send, agf_send, ag_recv, agf_recv, rs_send, far_recv, sum_recv, dir_recv,
):
    n = 4
    rows, dim = x_ref.shape
    r = rows // 2
    ff = wg_ref.shape[1]
    nk = dim // KC
    nb1 = ff // (2 * NU)
    kd = ff // KC
    npair = dim // (2 * NU)
    nt = 2 * npair
    me = lax.axis_index("tp")
    right, left = {"tp": lax.rem(me + 1, n)}, {"tp": lax.rem(me + n - 1, n)}
    mesh_id = pl.DeviceIdType.MESH

    def m(v, k):
        return pl.multiple_of(v, k)

    def put(ref, k, c, slot):
        pltpu.make_async_copy(
            ref.at[pl.ds(m(k * KC, KC), KC), pl.ds(m(c * NU, NU), NU)], wbuf.at[slot], wsem.at[slot]
        ).start()

    def start_up(h, kc, nb, j):
        slot = lax.rem(10 * h + 4 * nb + j, RING)
        put(wg_ref if j % 2 == 0 else wu_ref, kc, 2 * nb + j // 2, slot)

    def start_down(h, q):
        put(wd_ref, lax.rem(q, kd), q // kd, lax.rem(10 * h + q, RING))

    def await_slot(slot):
        pltpu.make_async_copy(wg_ref.at[pl.ds(0, KC), pl.ds(0, NU)], wbuf.at[slot], wsem.at[slot]).wait()

    def cut(k):
        return k // nk, pl.ds(m(lax.rem(k, nk) * KC, KC), KC)

    def ag_own(k, d):
        h, cols = cut(k)
        return pltpu.make_async_remote_copy(
            src_ref=x_ref.at[pl.ds(m(h * r, r), r), cols],
            dst_ref=xbuf.at[h, pl.ds((3 if d == 0 else 1) * r, r), cols],
            send_sem=ag_send.at[d], recv_sem=ag_recv.at[d, k],
            device_id=right if d == 0 else left, device_id_type=mesh_id)

    def ag_fwd(k, d):
        h = k // nk
        cols = pl.ds(m(lax.rem(k, nk) * KC + d * (KC // 2), KC // 2), KC // 2)
        return pltpu.make_async_remote_copy(
            src_ref=xbuf.at[h, pl.ds((3 if d == 0 else 1) * r, r), cols],
            dst_ref=xbuf.at[h, pl.ds(2 * r, r), cols],
            send_sem=agf_send.at[d], recv_sem=agf_recv.at[d, k],
            device_id=right if d == 0 else left, device_id_type=mesh_id)

    def ag_start(k):
        for d in range(2):
            ag_own(k, d).start()

    def ag_point(k, last=False):
        for d in range(2):
            ag_own(k, d).wait_recv()
            ag_fwd(k, d).start()
        if not last:
            ag_start(k + 2)

    def rs_copy(kind, h, t, c):
        src, dst, sem = ((sfar, rfar, far_recv), (ssum, rsum, sum_recv), (sdir, rdir, dir_recv))[kind]
        to_right = (c == 0) != (kind == 2)
        i = h * nt + t
        return pltpu.make_async_remote_copy(
            src_ref=src.at[t], dst_ref=dst.at[i], send_sem=rs_send.at[kind], recv_sem=sem.at[i],
            device_id=right if to_right else left, device_id_type=mesh_id)

    def rs_start(kind, h, p):
        for c in range(2):
            rs_copy(kind, h, 2 * p + c, c).start()

    def rs_pass(h, p):
        for c in range(2):
            t = 2 * p + c
            rs_copy(0, h, t, c).wait_recv()
            ssum[t] = (thru[t] + rfar[h * nt + t].astype(F32)).astype(BF16)
        rs_start(1, h, p)

    def rs_final(h, p):
        for c in range(2):
            t = 2 * p + c
            i = h * nt + t
            rs_copy(1, h, t, c).wait_recv()
            rs_copy(2, h, t, c).wait_recv()
            cols = pl.ds(m(t * NU, NU), NU)
            rws = pl.ds(m(h * r, r), r)
            obuf[rws, cols] = (own[t] + rsum[i].astype(F32) + rdir[i].astype(F32)).astype(BF16)
        cols = pl.ds(m(2 * p * NU, 2 * NU), 2 * NU)
        pltpu.make_async_copy(obuf.at[rws, cols], out_ref.at[rws, cols], osem).start()

    def rs_sent():
        for kind, buf in enumerate((sfar, ssum, sdir)):
            pltpu.make_async_copy(buf, buf, rs_send.at[kind]).wait()

    for nb in range(nb1):
        for j in range(4):
            start_up(0, 0, nb, j)
    for h in range(2):
        pltpu.make_async_copy(x_ref.at[pl.ds(h * r, r)], xbuf.at[h, pl.ds(0, r)], xsem.at[h]).start()
    if COMM:
        barrier = pltpu.get_barrier_semaphore()
        for d in (left, right):
            pl.semaphore_signal(barrier, inc=1, device_id=d, device_id_type=mesh_id)
        pl.semaphore_wait(barrier, 2)
        ag_start(0)
        ag_start(1)
        ag_point(0)
        ag_point(1)
    for h in range(2):
        pltpu.make_async_copy(x_ref.at[pl.ds(h * r, r)], xbuf.at[h, pl.ds(0, r)], xsem.at[h]).wait()

    def half(h, _):
        def up_body(kc, nb, first, last):
            for j in range(4):
                await_slot(lax.rem(10 * h + 4 * nb + j, RING))
            xk = xbuf[h, :, pl.ds(m(kc * KC, KC), KC)]
            for c in range(2):
                cols = pl.ds(m(nb * 2 * NU + c * NU, NU), NU)
                s0 = lax.rem(10 * h + 4 * nb + 2 * c, RING)
                s1 = lax.rem(10 * h + 4 * nb + 2 * c + 1, RING)
                g = jnp.dot(xk, wbuf[s0], preferred_element_type=F32)
                u = jnp.dot(xk, wbuf[s1], preferred_element_type=F32)
                if not first:
                    g = acc_g[:, cols] + g
                    u = acc_u[:, cols] + u
                if last:
                    hid[:, cols] = (jax.nn.silu(g) * u).astype(BF16)
                else:
                    acc_g[:, cols] = g
                    acc_u[:, cols] = u
            for j in range(4):
                if last:
                    start_down(h, 4 * nb + j)
                else:
                    start_up(h, kc + 1, nb, j)
            if COMM:
                b = kc * nb1 + nb

                @pl.when((h == 0) & (lax.rem(b, 4) == 2))
                def _():
                    ag_point(b // 4 + 2)

                @pl.when((h == 1) & (lax.rem(b, 4) == 0) & (b >= 4) & (b < 4 + 4 * npair))
                def _():
                    rs_pass(0, b // 4 - 1)

                @pl.when((h == 1) & (lax.rem(b, 4) == 2) & (b >= 10) & (b < 10 + 4 * npair))
                def _():
                    rs_final(0, (b - 10) // 4)

        def chunk(kc, first, last):
            if COMM:
                for d in range(2):
                    ag_fwd(h * nk + kc, d).wait_recv()

            def one(nb, _):
                up_body(kc, nb, first, last)
                return 0

            lax.fori_loop(0, nb1, one, 0)

        chunk(0, True, False)

        def mid(kc, _):
            chunk(kc, False, False)
            return 0

        lax.fori_loop(1, nk - 1, mid, 0)
        chunk(nk - 1, False, True)

        if COMM:
            @pl.when(h == 1)
            def _():
                rs_sent()

        def down(p, _):
            for i in range(2 * kd):
                await_slot(lax.rem(10 * h + 10 * p + i, RING))
            for c in range(2):
                t = 2 * p + c
                y = jnp.dot(hid[:, :KC], wbuf[lax.rem(10 * h + 10 * p + 5 * c, RING)], preferred_element_type=F32)
                for k in range(1, kd):
                    y += jnp.dot(hid[:, k * KC:(k + 1) * KC], wbuf[lax.rem(10 * h + 10 * p + 5 * c + k, RING)],
                                 preferred_element_type=F32)
                own[t] = y[:r]
                sfar[t] = y[2 * r:3 * r].astype(BF16)
                thru[t] = y[r:2 * r] if c == 0 else y[3 * r:]
                sdir[t] = (y[3 * r:] if c == 0 else y[r:2 * r]).astype(BF16)
            if COMM:
                rs_start(0, h, p)

            @pl.when(p < npair - 2)
            def _():
                for i in range(2 * kd):
                    start_down(h, 10 * (p + 2) + i)

            @pl.when((p >= npair - 2) & (h == 0))
            def _():
                for i in range(2 * kd):
                    q = 10 * (p - (npair - 2)) + i
                    slot = lax.rem(10 + q, RING)
                    put(wg_ref if i % 2 == 0 else wu_ref, 0, q // 2, slot)

            if COMM:
                @pl.when((h == 0) | (p == 0))
                def _():
                    rs_start(2, h, p)

                @pl.when((h == 0) & (p == 0))
                def _():
                    ag_point(11)

                @pl.when((h == 0) & ((p == 2) | (p == 3)))
                def _():
                    ag_point(10 + p, last=True)

                @pl.when((h == 1) & (p >= 1))
                def _():
                    rs_pass(1, p - 1)
            return 0

        lax.fori_loop(0, npair, down, 0)
        return 0

    lax.fori_loop(0, 2, half, 0)

    if COMM:
        rs_start(2, 1, 1)
        rs_start(2, 1, 2)
        rs_pass(1, npair - 1)
        for p in range(3, npair):
            rs_start(2, 1, p)

        def fin(p, _):
            rs_final(1, p)
            return 0

        lax.fori_loop(0, npair, fin, 0)
        rs_sent()
        for d in range(2):
            pltpu.make_async_copy(x_ref, x_ref, ag_send.at[d]).wait()
            half_x = x_ref.at[:, pl.ds(0, dim // 2)]
            pltpu.make_async_copy(half_x, half_x, agf_send.at[d]).wait()
        pltpu.make_async_copy(obuf, out_ref, osem).wait()
    else:
        obuf[...] = jnp.zeros_like(obuf)
        obuf[:r, :NU] = own[0].astype(BF16)
        c = pltpu.make_async_copy(obuf, out_ref, osem)
        c.start()
        c.wait()


def solution(mesh):
    def step(x, w_gate, w_up, w_down):
        rows, dim = x.shape
        ff = w_gate.shape[1]
        r, nt = rows // 2, dim // NU
        n = mesh.shape["tp"]
        nag = 2 * (dim // KC)
        vm, dma = pltpu.VMEM, pltpu.SemaphoreType.DMA
        return pl.pallas_call(
            _kernel,
            out_shape=jax.ShapeDtypeStruct((rows, dim), BF16),
            in_specs=[pl.BlockSpec(memory_space=pl.ANY)] * 4,
            out_specs=pl.BlockSpec(memory_space=pl.ANY),
            scratch_shapes=[
                vm((2, n * r, dim), BF16),
                vm((n * r, ff), F32),
                vm((n * r, ff), F32),
                vm((n * r, ff), BF16),
                vm((RING, KC, NU), BF16),
                vm((nt, r, NU), F32),
                vm((nt, r, NU), F32),
                vm((rows, dim), BF16),
                vm((2 * nt, r, NU), BF16),
                vm((2 * nt, r, NU), BF16),
                vm((2 * nt, r, NU), BF16),
                vm((nt, r, NU), BF16),
                vm((nt, r, NU), BF16),
                vm((nt, r, NU), BF16),
                dma((RING,)),
                dma((2,)),
                dma,
                dma((2,)),
                dma((2,)),
                dma((2, nag)),
                dma((2, nag)),
                dma((3,)),
                dma((2 * nt,)),
                dma((2 * nt,)),
                dma((2 * nt,)),
            ],
            compiler_params=pltpu.CompilerParams(
                collective_id=0 if COMM else None, has_side_effects=True, vmem_limit_bytes=67043328),
        )(x, w_gate, w_up, w_down)

    return jax.shard_map(
        step, mesh=mesh,
        in_specs=(P(("dp", "tp"), None), P(None, "tp"), P(None, "tp"), P("tp", None)),
        out_specs=P(("dp", "tp"), None), check_vma=False)
```

```python
import jax
import jax.numpy as jnp
from jax import lax
from jax.experimental import pallas as pl
from jax.experimental.pallas import tpu as pltpu
from jax.sharding import PartitionSpec as P

F32 = jnp.float32
BF16 = jnp.bfloat16
KC = 1024
NU = 512
BODY = 10
RING = 2 * BODY
LAG = 4
COMM = True
DMA = True


def _kernel(
    x_ref, wg_ref, wu_ref, wd_ref, out_ref,
    xbuf, acc_g, acc_u, hid, wbuf, thru, own, rfar, rsum, rdir, sfar, ssum, sdir,
    wsem, xsem, ag_send, agf_send, ag_recv, agf_recv, rs_send, far_recv, sum_recv, dir_recv,
):
    n = 4
    rows, dim = x_ref.shape
    r = rows // 2
    ff = wg_ref.shape[1]
    nk = dim // KC
    nc = BODY // 2
    kd = ff // KC
    npair = dim // (2 * NU)
    nt = 2 * npair
    npc = dim // NU
    me = lax.axis_index("tp")
    right, left = {"tp": lax.rem(me + 1, n)}, {"tp": lax.rem(me + n - 1, n)}
    mesh_id = pl.DeviceIdType.MESH

    def m(v, k):
        return v if isinstance(v, int) else pl.multiple_of(v, k)

    def put(ref, k, c, slot):
        if DMA:
            pltpu.make_async_copy(
                ref.at[pl.ds(m(k * KC, KC), KC), pl.ds(m(c * NU, NU), NU)], wbuf.at[slot], wsem.at[slot]
            ).start()

    def put_up(h, kc, i, c):
        base = BODY * lax.rem(i + h, 2)
        for j, ref in enumerate((wg_ref, wu_ref)):
            put(ref, kc, nc * i + c, base + 2 * c + j)

    def put_down(h, p, idx):
        put(wd_ref, idx % kd, 2 * p + idx // kd, BODY * lax.rem(p + h, 2) + idx)

    def await_slot(slot):
        if DMA:
            pltpu.make_async_copy(wg_ref.at[pl.ds(0, KC), pl.ds(0, NU)], wbuf.at[slot], wsem.at[slot]).wait()

    def ag_own(s, d):
        h = s // npc
        cols = pl.ds(m((s % npc) * NU, NU), NU)
        return pltpu.make_async_remote_copy(
            src_ref=x_ref.at[pl.ds(m(h * r, r), r), cols],
            dst_ref=xbuf.at[h, pl.ds((3 if d == 0 else 1) * r, r), cols],
            send_sem=ag_send.at[d], recv_sem=ag_recv.at[d, s],
            device_id=right if d == 0 else left, device_id_type=mesh_id)

    def ag_fwd(s, d):
        h = s // npc
        cols = pl.ds(m((s % npc) * NU + d * (NU // 2), NU // 2), NU // 2)
        return pltpu.make_async_remote_copy(
            src_ref=xbuf.at[h, pl.ds((3 if d == 0 else 1) * r, r), cols],
            dst_ref=xbuf.at[h, pl.ds(2 * r, r), cols],
            send_sem=agf_send.at[d], recv_sem=agf_recv.at[d, s],
            device_id=right if d == 0 else left, device_id_type=mesh_id)

    def ag_start(s):
        if COMM:
            for d in range(2):
                ag_own(s, d).start()

    def ag_pass(s):
        if COMM:
            for d in range(2):
                ag_own(s, d).wait_recv()
                ag_fwd(s, d).start()

    def ag_done(s):
        if COMM:
            for d in range(2):
                ag_fwd(s, d).wait_recv()

    FAR, SUM, DIR = range(3)

    def rs_copy(kind, h, p, c):
        src, dst, sem = ((sfar, rfar, far_recv), (ssum, rsum, sum_recv), (sdir, rdir, dir_recv))[kind]
        to_right = (c == 0) != (kind == DIR)
        t = 2 * p + c
        i = h * nt + t
        return pltpu.make_async_remote_copy(
            src_ref=src.at[t], dst_ref=dst.at[i], send_sem=rs_send.at[kind], recv_sem=sem.at[i],
            device_id=right if to_right else left, device_id_type=mesh_id)

    def rs_start(kind, h, p, c):
        if COMM:
            rs_copy(kind, h, p, c).start()

    def rs_pass(h, p, c):
        t = 2 * p + c
        rs_copy(FAR, h, p, c).wait_recv()
        ssum[t] = (thru[t] + rfar[h * nt + t].astype(F32)).astype(BF16)
        rs_start(SUM, h, p, c)

    def rs_final(h, p):
        for c in range(2):
            t = 2 * p + c
            i = h * nt + t
            rs_copy(SUM, h, p, c).wait_recv()
            rs_copy(DIR, h, p, c).wait_recv()
            out_ref[pl.ds(h * r, r), pl.ds(m(t * NU, NU), NU)] = (
                own[t] + rsum[i].astype(F32) + rdir[i].astype(F32)).astype(BF16)

    def rs_sent():
        for kind, buf in enumerate((sfar, ssum, sdir)):
            pltpu.make_async_copy(buf, buf, rs_send.at[kind]).wait()

    if COMM:
        barrier = pltpu.get_barrier_semaphore()
        for d in (left, right):
            pl.semaphore_signal(barrier, inc=1, device_id=d, device_id_type=mesh_id)
    for c in range(nc):
        put_up(0, 0, 0, c)
    for h in range(2):
        pltpu.make_async_copy(x_ref.at[pl.ds(h * r, r)], xbuf.at[h, pl.ds(0, r)], xsem.at[h]).start()
    if COMM:
        pl.semaphore_wait(barrier, 2)
    ag_start(0)
    ag_start(1)
    for c in range(nc):
        put_up(0, 0, 1, c)
    ag_pass(0)
    ag_start(2)
    ag_pass(1)
    ag_start(3)
    for h in range(2):
        pltpu.make_async_copy(x_ref.at[pl.ds(h * r, r)], xbuf.at[h, pl.ds(0, r)], xsem.at[h]).wait()

    def up_step(h, kc, i, depth, first, last, refill, wait):
        base = BODY * lax.rem(i + h, 2)
        off, size = depth
        xk = xbuf[h, :, pl.ds(m(kc * KC + off, size), size)]

        def ready(c):
            if wait and c < nc:
                await_slot(base + 2 * c)
                await_slot(base + 2 * c + 1)

        def refill_tile(c):
            if refill == "up":
                put_up(h, kc + 1, i, c)
            elif refill == "down":
                for j in range(2):
                    put_down(h, i, 2 * c + j)

        for c in range(nc):
            ready(c)
        for c in range(nc):
            cols = pl.ds(m((nc * i + c) * NU, NU), NU)
            g = jnp.dot(xk, wbuf[base + 2 * c, pl.ds(off, size)], preferred_element_type=F32)
            u = jnp.dot(xk, wbuf[base + 2 * c + 1, pl.ds(off, size)], preferred_element_type=F32)
            if not first:
                g = acc_g[:, cols] + g
                u = acc_u[:, cols] + u
            if last:
                hid[:, cols] = (jax.nn.silu(g) * u).astype(BF16)
            else:
                acc_g[:, cols] = g
                acc_u[:, cols] = u
            if refill and c >= 1:
                refill_tile(c - 1)
        if refill:
            refill_tile(nc - 1)

    def loop(lo, hi, body):
        def step(i, _):
            body(i)
            return 0
        lax.fori_loop(lo, hi, step, 0)

    def rs_between(b):
        if not COMM:
            return

        @pl.when((b >= 1) & (b <= npair))
        def _():
            for c in range(2):
                rs_pass(0, b - 1, c)

        @pl.when((b >= 2 * nk - npair) & (b < 2 * nk))
        def _():
            rs_final(0, b - (2 * nk - npair))

    for h in range(2):
        if h == 0:
            ag_done(0)

            def first_a(i):
                up_step(0, 0, i, (0, KC // 2), True, False, None, True)
                ag_pass(2 + i)
                ag_start(4 + i)
            loop(0, 2, first_a)
            ag_done(1)

            def first_b(i):
                up_step(0, 0, i, (KC // 2, KC // 2), False, False, "up", False)
                ag_start(6 + i)
            loop(0, 2, first_b)

            def mid(kc, last=False):
                ag_done(2 * kc)
                ag_done(2 * kc + 1)
                q = 4 + 3 * (kc - 1)

                def one(i):
                    up_step(0, kc, i, (0, KC), False, last, "down" if last else "up", True)

                    @pl.when(i == 0)
                    def _():
                        ag_pass(q)
                        ag_pass(q + 1)
                        ag_start(q + LAG)
                        ag_start(q + LAG + 1)

                    @pl.when(i == 1)
                    def _():
                        ag_pass(q + 2)
                        ag_start(q + LAG + 2)
                loop(0, 2, one)
            loop(1, nk - 1, mid)
            mid(nk - 1, True)
            passed = 4 + 3 * (nk - 1)
        else:
            def chunk(kc, first, last):
                ag_done(npc + 2 * kc)
                ag_done(npc + 2 * kc + 1)

                def one(i):
                    up_step(1, kc, i, (0, KC), first, last, "down" if last else "up", True)
                    rs_between(2 * kc + i)
                loop(0, 2, one)

            chunk(0, True, False)
            loop(1, nk - 1, lambda kc: chunk(kc, False, False))
            chunk(nk - 1, False, True)
            if COMM:
                rs_sent()

        def down(p, tail):
            base = BODY * lax.rem(p + h, 2)
            for idx in range(kd):
                await_slot(base + idx)
            for c in range(2):
                if c == 0:
                    for idx in range(kd, 2 * kd):
                        await_slot(base + idx)
                y = None
                for k in range(kd):
                    z = jnp.dot(hid[:, k * KC:(k + 1) * KC], wbuf[base + c * kd + k], preferred_element_type=F32)
                    y = z if y is None else y + z
                t = 2 * p + c
                own[t] = y[:r]
                sfar[t] = y[2 * r:3 * r].astype(BF16)
                thru[t] = y[r:2 * r] if c == 0 else y[3 * r:]
                sdir[t] = (y[3 * r:] if c == 0 else y[r:2 * r]).astype(BF16)
                rs_start(FAR, h, p, c)
                if h == 0 or not tail:
                    rs_start(DIR, h, p, c)
                for idx in range(c * kd, (c + 1) * kd):
                    if not tail:
                        put_down(h, p + 2, idx)
                    elif h == 0:
                        put((wg_ref, wu_ref)[idx % 2], 0, nc * (p - (npair - 2)) + idx // 2,
                            BODY * lax.rem(p - (npair - 2) + 1, 2) + idx)
            if not COMM:
                return
            if h == 0:
                s = passed + p

                @pl.when(s < 2 * npc)
                def _():
                    ag_pass(s)

                @pl.when(s + LAG < 2 * npc)
                def _():
                    ag_start(s + LAG)
            else:
                @pl.when(p >= 1)
                def _():
                    rs_pass(1, p - 1, 0)

                @pl.when(p >= 2)
                def _():
                    rs_pass(1, p - 2, 1)

        loop(0, npair - 2, lambda p: down(p, False))
        loop(npair - 2, npair, lambda p: down(p, True))

    if COMM:
        rs_pass(1, npair - 2, 1)
        for c in range(2):
            rs_start(DIR, 1, npair - 2, c)
        for c in range(2):
            rs_pass(1, npair - 1, c)
        for c in range(2):
            rs_start(DIR, 1, npair - 1, c)
        loop(0, npair, lambda p: rs_final(1, p))
        rs_sent()
        for d in range(2):
            pltpu.make_async_copy(x_ref, x_ref, ag_send.at[d]).wait()
            half_x = x_ref.at[:, pl.ds(0, dim // 2)]
            pltpu.make_async_copy(half_x, half_x, agf_send.at[d]).wait()
    else:
        out_ref[:r, :NU] = own[0].astype(BF16)


def solution(mesh):
    def step(x, w_gate, w_up, w_down):
        rows, dim = x.shape
        ff = w_gate.shape[1]
        r, nt = rows // 2, dim // NU
        n = mesh.shape["tp"]
        vm, dma = pltpu.VMEM, pltpu.SemaphoreType.DMA
        return pl.pallas_call(
            _kernel,
            out_shape=pltpu.VMEM((rows, dim), BF16),
            in_specs=[pl.BlockSpec(memory_space=pl.ANY)] * 4,
            out_specs=pl.BlockSpec(memory_space=pltpu.VMEM),
            scratch_shapes=[
                vm((2, n * r, dim), BF16),
                vm((n * r, ff), F32),
                vm((n * r, ff), F32),
                vm((n * r, ff), BF16),
                vm((RING, KC, NU), BF16),
                vm((nt, r, NU), F32),
                vm((nt, r, NU), F32),
                vm((2 * nt, r, NU), BF16),
                vm((2 * nt, r, NU), BF16),
                vm((2 * nt, r, NU), BF16),
                vm((nt, r, NU), BF16),
                vm((nt, r, NU), BF16),
                vm((nt, r, NU), BF16),
                dma((RING,)),
                dma((2,)),
                dma((2,)),
                dma((2,)),
                dma((2, 2 * nt)),
                dma((2, 2 * nt)),
                dma((3,)),
                dma((2 * nt,)),
                dma((2 * nt,)),
                dma((2 * nt,)),
            ],
            compiler_params=pltpu.CompilerParams(
                collective_id=0 if COMM else None, has_side_effects=True, vmem_limit_bytes=67043328 - 2400000),
        )(x, w_gate, w_up, w_down)

    return jax.shard_map(
        step, mesh=mesh,
        in_specs=(P(("dp", "tp"), None), P(None, "tp"), P(None, "tp"), P("tp", None)),
        out_specs=P(("dp", "tp"), None), check_vma=False)
```

```python
import jax
import jax.numpy as jnp
from jax import lax
from jax.experimental import pallas as pl
from jax.experimental.pallas import tpu as pltpu
from jax.sharding import PartitionSpec as P

F32 = jnp.float32
BF16 = jnp.bfloat16
KC = 1024
NU = 512
BODY = 10
RING = 2 * BODY


def _kernel(
    x_ref, wg_ref, wu_ref, wd_ref, out_ref,
    xbuf, acc_g, acc_u, hid, wbuf, thru, own, rfar, rsum, rdir, sfar, ssum, sdir,
    wsem, xsem, ag_send, agf_send, ag_recv, agf_recv, rs_send, far_recv, sum_recv, dir_recv,
):
    n = 4
    rows, dim = x_ref.shape
    r = rows // 2
    ff = wg_ref.shape[1]
    nk = dim // KC
    nc = BODY // 2
    kd = ff // KC
    npair = dim // (2 * NU)
    nt = 2 * npair
    nw = nk + 2
    npc = nw + nk
    me = lax.axis_index("tp")
    right, left = {"tp": lax.rem(me + 1, n)}, {"tp": lax.rem(me + n - 1, n)}
    mesh_id = pl.DeviceIdType.MESH

    def m(v, k):
        return v if isinstance(v, int) else pl.multiple_of(v, k)

    def put(ref, k, c, side, idx):
        pltpu.make_async_copy(
            ref.at[pl.ds(m(k * KC, KC), KC), pl.ds(m(c * NU, NU), NU)], wbuf.at[side * BODY + idx], wsem.at[side]
        ).start()

    def put_up(h, kc, i, c):
        for j, ref in enumerate((wg_ref, wu_ref)):
            put(ref, kc, nc * i + c, lax.rem(i + h, 2), 2 * c + j)

    def put_down(h, p, idx):
        put(wd_ref, idx % kd, 2 * p + idx // kd, lax.rem(p + h, 2), idx)

    def await_tiles(side):
        tiles = wbuf.at[pl.ds(side * BODY, BODY)]
        pltpu.make_async_copy(tiles, tiles, wsem.at[side]).wait()

    def piece(s):
        if isinstance(s, int) and s < 4:
            return 0, s * NU, NU
        h = s // nw
        return h, (s - 2 - nk * h) * KC, KC

    def ag_own(s, d):
        h, c0, width = piece(s)
        cols = pl.ds(m(c0, NU), width)
        return pltpu.make_async_remote_copy(
            src_ref=x_ref.at[pl.ds(m(h * r, r), r), cols],
            dst_ref=xbuf.at[h, pl.ds((3 if d == 0 else 1) * r, r), cols],
            send_sem=ag_send.at[d], recv_sem=ag_recv.at[d, s],
            device_id=right if d == 0 else left, device_id_type=mesh_id)

    def ag_fwd(s, d):
        h, c0, width = piece(s)
        cols = pl.ds(m(c0 + d * (width // 2), NU // 2), width // 2)
        return pltpu.make_async_remote_copy(
            src_ref=xbuf.at[h, pl.ds((3 if d == 0 else 1) * r, r), cols],
            dst_ref=xbuf.at[h, pl.ds(2 * r, r), cols],
            send_sem=agf_send.at[d], recv_sem=agf_recv.at[d, s],
            device_id=right if d == 0 else left, device_id_type=mesh_id)

    def ag_start(s):
        for d in range(2):
            ag_own(s, d).start()

    def ag_pass(s):
        for d in range(2):
            ag_own(s, d).wait_recv()
            ag_fwd(s, d).start()

    def ag_done(s):
        for d in range(2):
            ag_fwd(s, d).wait_recv()

    FAR, SUM, DIR = range(3)

    def rs_copy(kind, h, p, c):
        src, dst, sem = ((sfar, rfar, far_recv), (ssum, rsum, sum_recv), (sdir, rdir, dir_recv))[kind]
        step = lax.rem(c, 2) if kind != DIR else 1 - lax.rem(c, 2)
        to = {"tp": lax.rem(me + 1 + (n - 2) * step, n)}
        t = 2 * p + c
        i = h * nt + t
        return pltpu.make_async_remote_copy(
            src_ref=src.at[t], dst_ref=dst.at[i], send_sem=rs_send.at[kind], recv_sem=sem.at[i],
            device_id=to, device_id_type=mesh_id)

    def rs_start(kind, h, p, c):
        rs_copy(kind, h, p, c).start()

    def rs_pass(h, p, c):
        t = 2 * p + c
        rs_copy(FAR, h, p, c).wait_recv()
        ssum[t] = (thru[t] + rfar[h * nt + t].astype(F32)).astype(BF16)
        rs_start(SUM, h, p, c)

    def put_own(h, p, c, value):
        if h == 0:
            own[2 * p + c] = value
        else:
            (acc_g, acc_u)[c][:r, pl.ds(m(p * NU, NU), NU)] = value

    def get_own(h, p, c):
        return own[2 * p + c] if h == 0 else (acc_g, acc_u)[c][:r, pl.ds(m(p * NU, NU), NU)]

    def rs_final(h, p):
        for c in range(2):
            t = 2 * p + c
            i = h * nt + t
            rs_copy(SUM, h, p, c).wait_recv()
            rs_copy(DIR, h, p, c).wait_recv()
            out_ref[pl.ds(h * r, r), pl.ds(m(t * NU, NU), NU)] = (
                get_own(h, p, c) + rsum[i].astype(F32) + rdir[i].astype(F32)).astype(BF16)

    def rs_sent(*kinds):
        for kind in kinds:
            buf = (sfar, ssum, sdir)[kind]
            pltpu.make_async_copy(buf, buf, rs_send.at[kind]).wait()

    barrier = pltpu.get_barrier_semaphore()
    for d in (left, right):
        pl.semaphore_signal(barrier, inc=1, device_id=d, device_id_type=mesh_id)
    for h in range(2):
        pltpu.make_async_copy(x_ref.at[pl.ds(h * r, r)], xbuf.at[h, pl.ds(0, r)], xsem.at[h]).start()
    pl.semaphore_wait(barrier, 2)
    ag_start(0)
    ag_start(1)
    for c in range(nc):
        put_up(0, 0, 0, c)
    ag_pass(0)
    ag_start(2)
    for c in range(nc):
        put_up(0, 0, 1, c)
    ag_pass(1)
    ag_start(3)
    for h in range(2):
        pltpu.make_async_copy(x_ref.at[pl.ds(h * r, r)], xbuf.at[h, pl.ds(0, r)], xsem.at[h]).wait()

    def up_step(h, kc, i, depth, first, last, refill, wait, tile=None):
        base = BODY * lax.rem(i + h, 2)
        off, size = depth
        xk = xbuf[h, :, pl.ds(m(kc * KC + off, size), size)]

        def refill_tile(c):
            if refill == "up":
                put_up(h, kc + 1, i, c)
            elif refill == "down":
                for j in range(2):
                    put_down(h, i, 2 * c + j)

        if wait:
            await_tiles(lax.rem(i + h, 2))
        if tile is not None:
            rs_copy(FAR, 0, 0, tile).wait_recv()
        for c in range(nc):
            cols = pl.ds(m((nc * i + c) * NU, NU), NU)
            g = jnp.dot(xk, wbuf[base + 2 * c, pl.ds(off, size)], preferred_element_type=F32)
            u = jnp.dot(xk, wbuf[base + 2 * c + 1, pl.ds(off, size)], preferred_element_type=F32)
            if not first:
                g = acc_g[:, cols] + g
                u = acc_u[:, cols] + u
            if last:
                hid[:, cols] = (jax.nn.silu(g) * u).astype(BF16)
            else:
                acc_g[:, cols] = g
                acc_u[:, cols] = u
            if tile is not None and c == 1:
                ssum[tile] = (thru[tile] + rfar[tile].astype(F32)).astype(BF16)
            if refill and c >= 1:
                refill_tile(c - 1)
        if refill:
            refill_tile(nc - 1)
        if tile is not None:
            rs_copy(SUM, 0, 0, tile).start()

    def loop(lo, hi, body):
        def step(i, _):
            body(i)
            return 0
        lax.fori_loop(lo, hi, step, 0)

    for h in range(2):
        if h == 0:
            ag_done(0)

            def first_a(i):
                up_step(0, 0, i, (0, KC // 2), True, False, None, True)

                @pl.when(i == 0)
                def _():
                    ag_pass(2)
                    ag_start(4)

                @pl.when(i == 1)
                def _():
                    ag_pass(3)
            loop(0, 2, first_a)
            ag_done(1)

            def first_b(i):
                up_step(0, 0, i, (KC // 2, KC // 2), False, False, "up", False)

                @pl.when(i == 0)
                def _():
                    ag_start(5)
            loop(0, 2, first_b)
            ag_done(2)
            ag_done(3)

            def mid(kc, last=False):
                if last or not isinstance(kc, int):
                    @pl.when(kc > 1)
                    def _():
                        ag_done(kc + 2)

                def one(i):
                    up_step(0, kc, i, (0, KC), False, last, "down" if last else "up", True)
                    j = 2 * (kc - 1) + i
                    s = 4 + 2 * (j // 3) + lax.rem(j, 3)

                    @pl.when(lax.rem(j, 3) < 2)
                    def _():
                        ag_pass(s)
                        ag_start(s + 2)
                loop(0, 2, one)
            loop(1, nk - 1, mid)
            mid(jnp.int32(nk - 1), True)
            passed = 4 + 2 * (2 * (nk - 1) // 3)
        else:
            def chunk(kc, first, last):
                ag_done(nw + kc)

                def one(i):
                    up_step(1, kc, i, (0, KC), first, last, "down" if last else "up", True, tile=2 * kc + i)
                loop(0, 2, one)

            chunk(0, True, False)
            loop(1, nk - 1, lambda kc: chunk(kc, False, False))
            chunk(nk - 1, False, True)
            rs_sent(FAR, DIR)

        def down(p, tail):
            base = BODY * lax.rem(p + h, 2)
            await_tiles(lax.rem(p + h, 2))
            for c in range(2):
                y = None
                for k in range(kd):
                    z = jnp.dot(hid[:, k * KC:(k + 1) * KC], wbuf[base + c * kd + k], preferred_element_type=F32)
                    y = z if y is None else y + z
                t = 2 * p + c
                put_own(h, p, c, y[:r])
                sfar[t] = y[2 * r:3 * r].astype(BF16)
                thru[t] = y[r:2 * r] if c == 0 else y[3 * r:]
                sdir[t] = (y[3 * r:] if c == 0 else y[r:2 * r]).astype(BF16)
                rs_start(FAR, h, p, c)
                if h == 0 or not tail:
                    rs_start(DIR, h, p, c)
                for idx in range(c * kd, (c + 1) * kd):
                    if not tail:
                        put_down(h, p + 2, idx)
                    elif h == 0:
                        put((wg_ref, wu_ref)[idx % 2], 0, nc * (p - (npair - 2)) + idx // 2,
                            lax.rem(p - (npair - 2) + 1, 2), idx)
            if h == 0:
                @pl.when(p < 2)
                def _():
                    ag_pass(passed + p)
                    ag_start(passed + p + 2)

                @pl.when((p == 3) | (p == 5))
                def _():
                    ag_pass(passed + 2 + (p - 3) // 2)
            else:
                @pl.when(p == 1)
                def _():
                    rs_sent(SUM)

                @pl.when(p >= 1)
                def _():
                    rs_pass(1, p - 1, 0)

                @pl.when(p >= 2)
                def _():
                    rs_pass(1, p - 2, 1)

        loop(0, npair - 2, lambda p: down(p, False))
        loop(npair - 2, npair, lambda p: down(p, True))

    rs_pass(1, npair - 2, 1)
    for c in range(2):
        rs_start(DIR, 1, npair - 2, c)
    loop(0, npair, lambda p: rs_final(0, p))
    for c in range(2):
        rs_pass(1, npair - 1, c)
    for c in range(2):
        rs_start(DIR, 1, npair - 1, c)
    loop(0, npair, lambda p: rs_final(1, p))
    rs_sent(FAR, SUM, DIR)
    for d in range(2):
        pltpu.make_async_copy(x_ref, x_ref, ag_send.at[d]).wait()
        half_x = x_ref.at[:, pl.ds(0, dim // 2)]
        pltpu.make_async_copy(half_x, half_x, agf_send.at[d]).wait()


def solution(mesh):
    def step(x, w_gate, w_up, w_down):
        rows, dim = x.shape
        ff = w_gate.shape[1]
        r, nt = rows // 2, dim // NU
        n = mesh.shape["tp"]
        npc = 2 * (dim // KC) + 2
        vm, dma = pltpu.VMEM, pltpu.SemaphoreType.DMA
        return pl.pallas_call(
            _kernel,
            out_shape=pltpu.VMEM((rows, dim), BF16),
            in_specs=[pl.BlockSpec(memory_space=pl.ANY)] * 4,
            out_specs=pl.BlockSpec(memory_space=pltpu.VMEM),
            scratch_shapes=[
                vm((2, n * r, dim), BF16),
                vm((n * r, ff), F32),
                vm((n * r, ff), F32),
                vm((n * r, ff), BF16),
                vm((RING, KC, NU), BF16),
                vm((nt, r, NU), F32),
                vm((nt, r, NU), F32),
                vm((2 * nt, r, NU), BF16),
                vm((2 * nt, r, NU), BF16),
                vm((2 * nt, r, NU), BF16),
                vm((nt, r, NU), BF16),
                vm((nt, r, NU), BF16),
                vm((nt, r, NU), BF16),
                dma((2,)),
                dma((2,)),
                dma((2,)),
                dma((2,)),
                dma((2, npc)),
                dma((2, npc)),
                dma((3,)),
                dma((2 * nt,)),
                dma((2 * nt,)),
                dma((2 * nt,)),
            ],
            compiler_params=pltpu.CompilerParams(
                collective_id=0, has_side_effects=True, vmem_limit_bytes=67043328 - 2 * rows * dim),
        )(x, w_gate, w_up, w_down)

    return jax.shard_map(
        step, mesh=mesh,
        in_specs=(P(("dp", "tp"), None), P(None, "tp"), P(None, "tp"), P("tp", None)),
        out_specs=P(("dp", "tp"), None), check_vma=False)
```
